32 devices in a mesh: rows: 8 (over z, x), cols: 4 (over y, core).
Axes of the slice: x: 2, y: 2, z: 4, core: 2. Of those that a mesh axis runs over, the one named last changes fastest.
Arguments:
- tables: float32 [4, 4096, 512], P(None, 'rows', 'cols'), may hold values from -1.5 to 1.5
- dense_features: float32 [256, 512], P('rows', 'cols'), may hold values from -6 to 6
- slot_rows: int32 [8, 8, 4, 64], P('rows'), may hold values from 0 to 511, as said below
- slot_examples: int32 [8, 8, 4, 64], P('rows'), may hold values from 0 to 31, as said below
- slot_counts: int32 [8, 8, 4], P('rows'), may hold values from 21 to 64, as said below
Outputs:
- pooled: float32 [256, 4, 512], P('rows', None, 'cols')
- interactions: float32 [256, 10], P('rows')
The draws below stay inside these ranges and needn't reach their ends.
Inputs may be any that keep to these rules, and one draw needn't show every extreme that they name: slot_rows[s, o, t, c] names row o * 512 + value of table t. `slot_examples`: an example of the source device s. `slot_counts`: slots 0 to count - 1 of a bucket are live, the others unused; some bucket of every draw is full.
All inputs are finite; a program needn't handle non-finite values.
Results may differ from the reference program's by a relative error of at most 0.0003.
Values sent between devices are 32-bit elements; how exact they have to be, the bound alone decides.
A program may use at most 64 MiB of HBM per device.

```python
import jax
import jax.numpy as jnp
import numpy as np
from jax import lax

E = 512
TABLES = 4
ROWS_DEV = 512
B_DEV = 32
CAP = 64
BATCH = 256
TABLE_ROWS = 4096
N_ROWS = 8


def draw_slot_counts(key, part):
    first_key, second_key = jax.random.split(jax.random.fold_in(key, 11))
    base = jax.random.randint(first_key, (N_ROWS, N_ROWS, TABLES), CAP // 3, 2 * CAP // 3 + 1)
    hottest = jax.random.randint(second_key, (TABLES,), 0, N_ROWS)
    is_hot = jnp.arange(N_ROWS)[None, :, None] == hottest[None, None, :]
    return jnp.where(is_hot, CAP, base).astype(jnp.int32)


def draw_slot_rows(key, part):
    first_key, second_key, third_key = jax.random.split(jax.random.fold_in(key, 23), 3)
    shape_all = (N_ROWS, N_ROWS, TABLES, CAP)
    first_draw = jax.random.randint(first_key, shape_all, 0, ROWS_DEV)
    second_draw = jax.random.randint(second_key, shape_all, 0, ROWS_DEV)
    offsets = jax.random.randint(third_key, (N_ROWS, TABLES), 0, ROWS_DEV)
    skewed = first_draw * second_draw // ROWS_DEV
    return ((skewed + offsets[None, :, :, None]) % ROWS_DEV).astype(jnp.int32)


def draw_slot_examples(key, part):
    first_key, second_key = jax.random.split(jax.random.fold_in(key, 37))
    shape_all = (N_ROWS, N_ROWS, TABLES, CAP)
    first_draw = jax.random.randint(first_key, shape_all, 0, B_DEV)
    second_draw = jax.random.randint(second_key, shape_all, 0, B_DEV)
    return jnp.minimum(first_draw, second_draw).astype(jnp.int32)


def shard_levels(key, dims, cuts, least, top_value):
    def one(axis_at, blocks):
        heights = jax.random.uniform(jax.random.fold_in(jax.random.fold_in(key, 6), axis_at), (blocks,), jnp.float32, least / len(cuts), top_value / len(cuts))
        return jnp.repeat(jnp.exp(heights), dims[axis_at] // blocks).reshape((-1,) + (1,) * (len(dims) - axis_at - 1))

    factor_of = one(*cuts[0])
    for cut in cuts[1:]:
        factor_of = factor_of * one(*cut)
    return factor_of


def bell_draw(rng, extent, width, most, cuts=(), kind=jnp.bfloat16):
    array = jax.random.normal(rng, extent, jnp.float32) * width
    if len(cuts) > 0:
        array = shard_levels(rng, extent, cuts, -0.22, 0.18) * array
    return jnp.clip(array, min=-most, max=most).astype(kind)


def setup_inputs(seed: int = 0) -> dict:
    keys = jax.random.split(jax.random.key(seed), 6)
    tables = bell_draw(keys[0], (TABLES, TABLE_ROWS, E), 0.25, 1.5, ((1, 8), (2, 4)), jnp.float32)
    dense_features = bell_draw(keys[1], (BATCH, E), 1.0, 6.0, ((0, 8), (1, 4)), jnp.float32)
    slot_rows = draw_slot_rows(jax.random.fold_in(keys[5], 71), 0)
    slot_examples = draw_slot_examples(jax.random.fold_in(keys[5], 71), 0)
    slot_counts = draw_slot_counts(jax.random.fold_in(keys[5], 71), 0)
    return {"tables": tables, "dense_features": dense_features, "slot_rows": slot_rows, "slot_examples": slot_examples, "slot_counts": slot_counts}


def reference(tables, dense_features, slot_rows, slot_examples, slot_counts):
    slot_index = jnp.arange(CAP, dtype=jnp.int32)
    live_slots = slot_index[None, None, None, :] < slot_counts[:, :, :, None]
    owner_base = (jnp.arange(N_ROWS, dtype=jnp.int32) * ROWS_DEV)[:, None, None]
    table_index = jnp.arange(TABLES, dtype=jnp.int32)[None, :, None]

    def one_source(pieces):
        rows_here, examples_here, live_here = pieces
        global_rows = (rows_here + owner_base).astype(jnp.int32)
        looked = tables[table_index, global_rows]
        looked = jnp.where(live_here[:, :, :, None], looked, jnp.zeros_like(looked))
        segment_ids = (examples_here * TABLES + table_index).astype(jnp.int32)
        summed = jax.ops.segment_sum(looked.reshape(-1, E), segment_ids.reshape(-1), num_segments=B_DEV * TABLES)
        return summed.reshape(B_DEV, TABLES, E)

    pooled = lax.map(one_source, (slot_rows, slot_examples, live_slots)).reshape(BATCH, TABLES, E)
    vectors = jnp.concatenate([dense_features[:, None, :], pooled], axis=1)
    gram_matrix = jnp.einsum("bie,bje->bij", vectors, vectors, precision=lax.Precision.HIGHEST)
    pair_first, pair_second = np.triu_indices(TABLES + 1, 1)
    interactions = gram_matrix[:, pair_first, pair_second] * (E ** -0.5)
    return pooled, interactions
```

```python
import functools

import jax
import jax.numpy as jnp
from jax import lax
from jax.experimental import pallas as pl
from jax.experimental.pallas import tpu as pltpu
from jax.sharding import PartitionSpec as P

MESH = pl.DeviceIdType.MESH
DEAD = -65536


def kernel(
    n,
    cols,
    tables_hbm,
    dense_ref,
    rows_ref,
    examples_ref,
    counts_ref,
    pooled_ref,
    inter_ref,
    table_buf,
    split_buf,
    id_send,
    id_recv,
    pair_keep,
    pair_send,
    pair_recv,
    far_send,
    far_recv,
    gram_recv,
    gram_send,
    table_sem,
    id_ssem,
    id_rsem,
    pair_ssem,
    pair_rsem,
    far_ssem,
    far_rsem,
    gram_ssem,
    gram_rsem,
):
    tables, range_rows, width = table_buf.shape
    here = dense_ref.shape[0]
    cap = rows_ref.shape[3]
    far = n // 2
    me = lax.axis_index("rows")
    col = lax.axis_index("cols")
    hi, lo = me // 2, me % 2
    mate = hi * 2 + (1 - lo)

    load = pltpu.make_async_copy(tables_hbm, table_buf, table_sem)
    load.start()

    barrier = pltpu.get_barrier_semaphore()
    for j in range(1, n):
        pl.semaphore_signal(barrier, inc=1, device_id={"rows": (me + j) % n}, device_id_type=MESH)
    for j in range(1, cols):
        pl.semaphore_signal(barrier, inc=1, device_id={"cols": (col + j) % cols}, device_id_type=MESH)

    slot = lax.broadcasted_iota(jnp.int32, (tables, cap), 1)
    table_id = lax.broadcasted_iota(jnp.int32, (tables, cap), 0)
    for p in range(n):
        count = jnp.full((tables, cap), counts_ref[0, p, 0], jnp.int32)
        for t in range(1, tables):
            count = jnp.where(table_id == t, counts_ref[0, p, t], count)
        rows_p = rows_ref[0, p]
        ex_p = jnp.where(slot < count, examples_ref[0, p], DEAD)
        id_send[p, 0:tables, :] = jnp.concatenate([rows_p, rows_p], axis=1)
        id_send[p, tables : 2 * tables, :] = jnp.concatenate([ex_p, ex_p], axis=1)

    pl.semaphore_wait(barrier, n - 1 + cols - 1)

    def id_copy(dst):
        return pltpu.make_async_remote_copy(
            src_ref=id_send.at[dst],
            dst_ref=id_recv.at[me],
            send_sem=id_ssem.at[dst],
            recv_sem=id_rsem.at[me],
            device_id={"rows": dst},
            device_id_type=MESH,
        )

    def id_wait(src):
        pltpu.make_async_remote_copy(
            src_ref=id_send.at[src],
            dst_ref=id_recv.at[src],
            send_sem=id_ssem.at[src],
            recv_sem=id_rsem.at[src],
            device_id={"rows": src},
            device_id_type=MESH,
        ).wait_recv()

    for j in range(1, far):
        dst_hi = (hi + far - j) % far
        id_copy(dst_hi * 2 + lo).start()
        id_copy(dst_hi * 2 + (1 - lo)).start()
    id_copy(mate).start()
    id_recv[me] = id_send[me]

    load.wait()
    for t in range(tables):
        whole = table_buf[t]
        high = whole.astype(jnp.bfloat16)
        split_buf[t, :, 0:width] = high
        split_buf[t, :, width : 2 * width] = (whole - high.astype(jnp.float32)).astype(jnp.bfloat16)

    first_half = lax.broadcasted_iota(jnp.int32, (tables, 2 * cap), 1) < cap
    offset = jnp.where(first_half, lo * here, (1 - lo) * here)
    row_iota = lax.broadcasted_iota(jnp.int32, (range_rows, 2 * cap), 0)
    ex_iota = lax.broadcasted_iota(jnp.int32, (2 * here, 2 * cap), 0)

    def group_of(k):
        return (hi + 1 + k) % far

    def pair_copy(g):
        return pltpu.make_async_remote_copy(
            src_ref=pair_send.at[g],
            dst_ref=pair_recv.at[g],
            send_sem=pair_ssem.at[g],
            recv_sem=pair_rsem.at[g],
            device_id={"rows": mate},
            device_id_type=MESH,
        )

    def far_copy(g):
        return pltpu.make_async_remote_copy(
            src_ref=far_send.at[g],
            dst_ref=far_recv.at[hi],
            send_sem=far_ssem.at[g],
            recv_sem=far_rsem.at[hi],
            device_id={"rows": g * 2 + lo},
            device_id_type=MESH,
        )

    def far_wait(g):
        pltpu.make_async_remote_copy(
            src_ref=far_send.at[g],
            dst_ref=far_recv.at[g],
            send_sem=far_ssem.at[g],
            recv_sem=far_rsem.at[g],
            device_id={"rows": g * 2 + lo},
            device_id_type=MESH,
        ).wait_recv()

    def compute(g):
        even = id_recv[g * 2]
        odd = id_recv[g * 2 + 1]
        row_of = jnp.where(first_half, even[0:tables], odd[0:tables])
        code = jnp.where(first_half, even[tables : 2 * tables], odd[tables : 2 * tables]) + offset
        for t in range(tables):
            row_hot = jnp.where(row_iota == row_of[t : t + 1], 1.0, 0.0).astype(jnp.bfloat16)
            ex_hot = jnp.where(ex_iota == code[t : t + 1], 1.0, 0.0).astype(jnp.bfloat16)
            hits = lax.dot_general(
                ex_hot, row_hot, (((1,), (1,)), ((), ())), preferred_element_type=jnp.float32
            ).astype(jnp.bfloat16)
            both = jnp.dot(hits, split_buf[t], preferred_element_type=jnp.float32)
            part = both[:, 0:width] + both[:, width : 2 * width]
            pair_keep[g, t] = part[0:here]
            pair_send[g, t] = part[here : 2 * here]
        pair_copy(g).start()

    def forward(g):
        pair_copy(g).wait_recv()
        far_send[g] = pair_keep[g] + pair_recv[g]
        far_copy(g).start()

    def remote_group(g):
        id_wait(g * 2)
        id_wait(g * 2 + 1)
        compute(g)

    remote_group(group_of(0))
    if far <= 8:
        for k in range(1, far - 1):
            remote_group(group_of(k))
            forward(group_of(k - 1))
    else:

        @pl.loop(1, far - 1)
        def _(k):
            remote_group(group_of(k))
            forward(group_of(k - 1))

    id_wait(mate)
    compute(hi)
    forward(group_of(far - 2))

    pair_copy(hi).wait_recv()
    total = pair_keep[hi] + pair_recv[hi]
    for k in range(far - 1):
        g = (hi + far - 1 - k) % far
        far_wait(g)
        total = total + far_recv[g]

    vectors = [dense_ref[...]] + [total[t] for t in range(tables)]
    for t in range(tables):
        pooled_ref[:, t, :] = total[t]
    lane = lax.broadcasted_iota(jnp.int32, (here, 128), 1)
    gram = jnp.zeros((here, 128), jnp.float32)
    pair = 0
    for i in range(tables + 1):
        for j in range(i + 1, tables + 1):
            inner = jnp.sum(vectors[i] * vectors[j], axis=1, keepdims=True)
            gram = jnp.where(lane == pair, inner, gram)
            pair += 1
    gram_send[...] = gram
    gram_recv[col] = gram

    def gram_copy(j):
        return pltpu.make_async_remote_copy(
            src_ref=gram_send,
            dst_ref=gram_recv.at[col],
            send_sem=gram_ssem.at[j],
            recv_sem=gram_rsem.at[col],
            device_id={"cols": (col + j) % cols},
            device_id_type=MESH,
        )

    for j in range(1, cols):
        gram_copy(j).start()
    for j in range(1, cols):
        src = (col + j) % cols
        pltpu.make_async_remote_copy(
            src_ref=gram_send,
            dst_ref=gram_recv.at[src],
            send_sem=gram_ssem.at[j],
            recv_sem=gram_rsem.at[src],
            device_id={"cols": src},
            device_id_type=MESH,
        ).wait_recv()
    summed = gram_recv[0]
    for c in range(1, cols):
        summed = summed + gram_recv[c]
    inter_ref[...] = (summed * (width * cols) ** (-0.5))[:, 0:pair]

    for j in range(1, n):
        id_copy((me + j) % n).wait_send()
    for g in range(far):
        pair_copy(g).wait_send()
    for j in range(1, far):
        far_copy((hi + j) % far).wait_send()
    for j in range(1, cols):
        gram_copy(j).wait_send()


def body(n, cols, tables, dense_features, slot_rows, slot_examples, slot_counts):
    count, range_rows, width = tables.shape
    here = dense_features.shape[0]
    cap = slot_rows.shape[3]
    far = n // 2
    pairs = (count + 1) * count // 2
    vmem = pl.BlockSpec(memory_space=pltpu.VMEM)
    block = (far, count, here, width)
    return pl.pallas_call(
        functools.partial(kernel, n, cols),
        out_shape=(
            jax.ShapeDtypeStruct((here, count, width), jnp.float32),
            jax.ShapeDtypeStruct((here, pairs), jnp.float32),
        ),
        in_specs=[
            pl.BlockSpec(memory_space=pl.ANY),
            vmem,
            vmem,
            vmem,
            pl.BlockSpec(memory_space=pltpu.SMEM),
        ],
        out_specs=(vmem, vmem),
        scratch_shapes=[
            pltpu.VMEM((count, range_rows, width), jnp.float32),
            pltpu.VMEM((count, range_rows, 2 * width), jnp.bfloat16),
            pltpu.VMEM((n, 2 * count, 2 * cap), jnp.int32),
            pltpu.VMEM((n, 2 * count, 2 * cap), jnp.int32),
            pltpu.VMEM(block, jnp.float32),
            pltpu.VMEM(block, jnp.float32),
            pltpu.VMEM(block, jnp.float32),
            pltpu.VMEM(block, jnp.float32),
            pltpu.VMEM(block, jnp.float32),
            pltpu.VMEM((cols, here, 128), jnp.float32),
            pltpu.VMEM((here, 128), jnp.float32),
            pltpu.SemaphoreType.DMA,
            pltpu.SemaphoreType.DMA((n,)),
            pltpu.SemaphoreType.DMA((n,)),
            pltpu.SemaphoreType.DMA((far,)),
            pltpu.SemaphoreType.DMA((far,)),
            pltpu.SemaphoreType.DMA((far,)),
            pltpu.SemaphoreType.DMA((far,)),
            pltpu.SemaphoreType.DMA((cols,)),
            pltpu.SemaphoreType.DMA((cols,)),
        ],
        compiler_params=pltpu.CompilerParams(collective_id=0, has_side_effects=True),
    )(tables, dense_features, slot_rows, slot_examples, slot_counts)


def solution(mesh):
    placed = (
        P(None, "rows", "cols"),
        P("rows", "cols"),
        P("rows", None, None, None),
        P("rows", None, None, None),
        P("rows", None, None),
    )
    return jax.shard_map(
        functools.partial(body, mesh.shape["rows"], mesh.shape["cols"]),
        mesh=mesh,
        in_specs=placed,
        out_specs=(P("rows", None, "cols"), P("rows", None)),
        check_vma=False,
    )
```

```python
import functools

import jax
import jax.numpy as jnp
from jax import lax
from jax.experimental import pallas as pl
from jax.experimental.pallas import tpu as pltpu
from jax.sharding import PartitionSpec as P

MESH = pl.DeviceIdType.MESH
CHUNKS = 2
DEAD = -65536


def kernel(
    n,
    cols,
    tables_hbm,
    dense_hbm,
    rows_hbm,
    examples_hbm,
    counts_hbm,
    pooled_hbm,
    inter_ref,
    dense_ref,
    rows_ref,
    examples_ref,
    counts_ref,
    pooled_ref,
    table_buf,
    split_buf,
    id_send,
    id_recv,
    pair_keep,
    pair_send,
    pair_recv,
    far_send,
    far_recv,
    gram_recv,
    gram_send,
    load_sem,
    id_ssem,
    id_rsem,
    pair_ssem,
    pair_rsem,
    far_ssem,
    far_rsem,
    gram_ssem,
    gram_rsem,
    store_sem,
):
    tables, range_rows, width = table_buf.shape
    here = dense_ref.shape[0]
    cap = rows_ref.shape[3]
    far = n // 2
    chunks = pair_ssem.shape[1]
    step = tables // chunks
    me = lax.axis_index("rows")
    col = lax.axis_index("cols")
    hi, lo = me // 2, me % 2
    mate = hi * 2 + (1 - lo)

    sources = (counts_hbm, rows_hbm, examples_hbm, tables_hbm, dense_hbm)
    targets = (counts_ref, rows_ref, examples_ref, table_buf, dense_ref)
    loads = [pltpu.make_async_copy(a, b, load_sem.at[i]) for i, (a, b) in enumerate(zip(sources, targets))]

    barrier = pltpu.get_barrier_semaphore()
    for j in range(1, n):
        pl.semaphore_signal(barrier, inc=1, device_id={"rows": (me + j) % n}, device_id_type=MESH)
    for j in range(1, cols):
        pl.semaphore_signal(barrier, inc=1, device_id={"cols": (col + j) % cols}, device_id_type=MESH)

    for load in loads:
        load.start()

    slot = lax.broadcasted_iota(jnp.int32, (tables, cap), 1)
    table_id = lax.broadcasted_iota(jnp.int32, (tables, cap), 0)
    for load in loads[:3]:
        load.wait()
    for p in range(n):
        count = jnp.full((tables, cap), counts_ref[0, 0, p], jnp.int32)
        for t in range(1, tables):
            count = jnp.where(table_id == t, counts_ref[0, t, p], count)
        rows_p = rows_ref[0, p]
        ex_p = jnp.where(slot < count, examples_ref[0, p], DEAD)
        id_send[p, 0:tables, :] = jnp.concatenate([rows_p, rows_p], axis=1)
        id_send[p, tables : 2 * tables, :] = jnp.concatenate([ex_p, ex_p], axis=1)

    pl.semaphore_wait(barrier, n - 1 + cols - 1)

    high_half = (2 * hi) // far
    low_hi = hi * (1 - high_half) + (far - 1 - hi) * high_half

    def group_of(k):
        beyond = (2 * (far - 1) - k - low_hi) // far
        g = far - 2 - k + beyond
        return g * (1 - high_half) + (far - 1 - g) * high_half

    def id_copy(dst):
        return pltpu.make_async_remote_copy(
            src_ref=id_send.at[dst],
            dst_ref=id_recv.at[me],
            send_sem=id_ssem.at[dst],
            recv_sem=id_rsem.at[me],
            device_id={"rows": dst},
            device_id_type=MESH,
        )

    def id_wait(src):
        pltpu.make_async_remote_copy(
            src_ref=id_send.at[src],
            dst_ref=id_recv.at[src],
            send_sem=id_ssem.at[src],
            recv_sem=id_rsem.at[src],
            device_id={"rows": src},
            device_id_type=MESH,
        ).wait_recv()

    for k in range(far - 1):
        dst_hi = group_of(k)
        id_copy(dst_hi * 2 + lo).start()
        id_copy(dst_hi * 2 + (1 - lo)).start()
    id_copy(mate).start()
    id_recv[me] = id_send[me]

    loads[3].wait()
    for t in range(tables):
        whole = table_buf[t]
        high = whole.astype(jnp.bfloat16)
        split_buf[t, :, 0:width] = high
        split_buf[t, :, width : 2 * width] = (whole - high.astype(jnp.float32)).astype(jnp.bfloat16)

    first_half = lax.broadcasted_iota(jnp.int32, (tables, 2 * cap), 1) < cap
    offset = jnp.where(first_half, lo * here, (1 - lo) * here)
    row_iota = lax.broadcasted_iota(jnp.int32, (range_rows, 2 * cap), 0)
    ex_iota = lax.broadcasted_iota(jnp.int32, (2 * here, 2 * cap), 0)

    def pair_copy(g, c):
        piece = pl.ds(c * step, step)
        return pltpu.make_async_remote_copy(
            src_ref=pair_send.at[g, piece],
            dst_ref=pair_recv.at[g, piece],
            send_sem=pair_ssem.at[g, c],
            recv_sem=pair_rsem.at[g, c],
            device_id={"rows": mate},
            device_id_type=MESH,
        )

    def far_copy(g, c):
        piece = pl.ds(c * step, step)
        return pltpu.make_async_remote_copy(
            src_ref=far_send.at[g, piece],
            dst_ref=far_recv.at[hi, piece],
            send_sem=far_ssem.at[g, c],
            recv_sem=far_rsem.at[hi, c],
            device_id={"rows": g * 2 + lo},
            device_id_type=MESH,
        )

    def far_wait(g, c):
        piece = pl.ds(c * step, step)
        pltpu.make_async_remote_copy(
            src_ref=far_send.at[g, piece],
            dst_ref=far_recv.at[g, piece],
            send_sem=far_ssem.at[g, c],
            recv_sem=far_rsem.at[g, c],
            device_id={"rows": g * 2 + lo},
            device_id_type=MESH,
        ).wait_recv()

    def compute(g):
        even = id_recv[g * 2]
        odd = id_recv[g * 2 + 1]
        row_of = jnp.where(first_half, even[0:tables], odd[0:tables])
        code = jnp.where(first_half, even[tables : 2 * tables], odd[tables : 2 * tables]) + offset
        for t in range(tables):
            row_hot = jnp.where(row_iota == row_of[t : t + 1], 1.0, 0.0).astype(jnp.bfloat16)
            ex_hot = jnp.where(ex_iota == code[t : t + 1], 1.0, 0.0).astype(jnp.bfloat16)
            hits = lax.dot_general(
                ex_hot, row_hot, (((1,), (1,)), ((), ())), preferred_element_type=jnp.float32
            ).astype(jnp.bfloat16)
            both = jnp.dot(hits, split_buf[t], preferred_element_type=jnp.float32)
            part = both[:, 0:width] + both[:, width : 2 * width]
            pair_keep[g, t] = part[0:here]
            pair_send[g, t] = part[here : 2 * here]
            if (t + 1) % step == 0:
                pair_copy(g, t // step).start()

    def forward(g):
        for c in range(chunks):
            pair_copy(g, c).wait_recv()
            piece = pl.ds(c * step, step)
            far_send[g, piece] = pair_keep[g, piece] + pair_recv[g, piece]
            far_copy(g, c).start()

    def remote_group(g):
        id_wait(g * 2)
        id_wait(g * 2 + 1)
        compute(g)

    remote_group(group_of(0))
    if far <= 8:
        for k in range(1, far - 1):
            remote_group(group_of(k))
            forward(group_of(k - 1))
    else:

        @pl.loop(1, far - 1)
        def _(k):
            remote_group(group_of(k))
            forward(group_of(k - 1))

    id_wait(mate)
    compute(hi)
    forward(group_of(far - 2))

    for c in range(chunks):
        pair_copy(hi, c).wait_recv()
    total = pair_keep[hi] + pair_recv[hi]
    for k in range(far - 1):
        g = group_of(far - 2 - k)
        for c in range(chunks):
            far_wait(g, c)
        total = total + far_recv[g]

    for t in range(tables):
        pooled_ref[:, t, :] = total[t]
    store = pltpu.make_async_copy(pooled_ref, pooled_hbm, store_sem)
    store.start()
    loads[4].wait()
    vectors = [dense_ref[...]] + [total[t] for t in range(tables)]
    lane = lax.broadcasted_iota(jnp.int32, (here, 128), 1)
    gram = jnp.zeros((here, 128), jnp.float32)
    pair = 0
    for i in range(tables + 1):
        for j in range(i + 1, tables + 1):
            inner = jnp.sum(vectors[i] * vectors[j], axis=1, keepdims=True)
            gram = jnp.where(lane == pair, inner, gram)
            pair += 1
    gram = gram.T[0 : gram_send.shape[0]]
    gram_send[...] = gram
    gram_recv[col] = gram

    def gram_copy(j):
        return pltpu.make_async_remote_copy(
            src_ref=gram_send,
            dst_ref=gram_recv.at[col],
            send_sem=gram_ssem.at[j],
            recv_sem=gram_rsem.at[col],
            device_id={"cols": (col + j) % cols},
            device_id_type=MESH,
        )

    for j in range(1, cols):
        gram_copy(j).start()
    for j in range(1, cols):
        src = (col + j) % cols
        pltpu.make_async_remote_copy(
            src_ref=gram_send,
            dst_ref=gram_recv.at[src],
            send_sem=gram_ssem.at[j],
            recv_sem=gram_rsem.at[src],
            device_id={"cols": src},
            device_id_type=MESH,
        ).wait_recv()
    summed = gram_recv[0]
    for c in range(1, cols):
        summed = summed + gram_recv[c]
    inter_ref[...] = (summed * (width * cols) ** (-0.5))[0:pair]

    for j in range(1, n):
        id_copy((me + j) % n).wait_send()
    for c in range(chunks):
        for g in range(far):
            pair_copy(g, c).wait_send()
        for j in range(1, far):
            far_copy((hi + j) % far, c).wait_send()
    for j in range(1, cols):
        gram_copy(j).wait_send()
    store.wait()


def body(n, cols, tables, dense_features, slot_rows, slot_examples, slot_counts):
    count, range_rows, width = tables.shape
    here = dense_features.shape[0]
    cap = slot_rows.shape[3]
    far = n // 2
    pairs = (count + 1) * count // 2
    vmem = pl.BlockSpec(memory_space=pltpu.VMEM)
    block = (far, count, here, width)
    chunks = CHUNKS
    any_space = pl.BlockSpec(memory_space=pl.ANY)
    pair_rows = -(-pairs // 8) * 8
    pooled, inter = pl.pallas_call(
        functools.partial(kernel, n, cols),
        out_shape=(
            jax.ShapeDtypeStruct((here, count, width), jnp.float32),
            jax.ShapeDtypeStruct((pairs, here), jnp.float32),
        ),
        in_specs=[any_space] * 5,
        out_specs=(any_space, vmem),
        scratch_shapes=[
            pltpu.VMEM((here, width), jnp.float32),
            pltpu.VMEM(slot_rows.shape, jnp.int32),
            pltpu.VMEM(slot_rows.shape, jnp.int32),
            pltpu.SMEM((1, count, n), jnp.int32),
            pltpu.VMEM((here, count, width), jnp.float32),
            pltpu.VMEM((count, range_rows, width), jnp.float32),
            pltpu.VMEM((count, range_rows, 2 * width), jnp.bfloat16),
            pltpu.VMEM((n, 2 * count, 2 * cap), jnp.int32),
            pltpu.VMEM((n, 2 * count, 2 * cap), jnp.int32),
            pltpu.VMEM(block, jnp.float32),
            pltpu.VMEM(block, jnp.float32),
            pltpu.VMEM(block, jnp.float32),
            pltpu.VMEM(block, jnp.float32),
            pltpu.VMEM(block, jnp.float32),
            pltpu.VMEM((cols, pair_rows, here), jnp.float32),
            pltpu.VMEM((pair_rows, here), jnp.float32),
            pltpu.SemaphoreType.DMA((5,)),
            pltpu.SemaphoreType.DMA((n,)),
            pltpu.SemaphoreType.DMA((n,)),
            pltpu.SemaphoreType.DMA((far, chunks)),
            pltpu.SemaphoreType.DMA((far, chunks)),
            pltpu.SemaphoreType.DMA((far, chunks)),
            pltpu.SemaphoreType.DMA((far, chunks)),
            pltpu.SemaphoreType.DMA((cols,)),
            pltpu.SemaphoreType.DMA((cols,)),
            pltpu.SemaphoreType.DMA,
        ],
        compiler_params=pltpu.CompilerParams(collective_id=0, has_side_effects=True),
    )(tables, dense_features, slot_rows, slot_examples, slot_counts.transpose(0, 2, 1))
    return pooled, inter.T


def solution(mesh):
    placed = (
        P(None, "rows", "cols"),
        P("rows", "cols"),
        P("rows", None, None, None),
        P("rows", None, None, None),
        P("rows", None, None),
    )
    return jax.shard_map(
        functools.partial(body, mesh.shape["rows"], mesh.shape["cols"]),
        mesh=mesh,
        in_specs=placed,
        out_specs=(P("rows", None, "cols"), P("rows", None)),
        check_vma=False,
    )
```

```python
import functools

import jax
import jax.numpy as jnp
from jax import lax
from jax.experimental import pallas as pl
from jax.experimental.pallas import tpu as pltpu
from jax.sharding import PartitionSpec as P

MESH = pl.DeviceIdType.MESH
CHUNKS = 2
DEAD = -65536


def kernel(
    n,
    cols,
    tables_hbm,
    dense_hbm,
    rows_hbm,
    examples_hbm,
    counts_hbm,
    pooled_ref,
    inter_ref,
    dense_ref,
    rows_ref,
    examples_ref,
    counts_ref,
    table_buf,
    split_buf,
    id_send,
    id_recv,
    pair_keep,
    pair_send,
    pair_recv,
    far_send,
    far_recv,
    gram_recv,
    gram_send,
    load_sem,
    id_ssem,
    id_rsem,
    pair_ssem,
    pair_rsem,
    far_ssem,
    far_rsem,
    gram_ssem,
    gram_rsem,
):
    tables, range_rows, width = table_buf.shape
    here = dense_ref.shape[0]
    cap = rows_ref.shape[3]
    far = n // 2
    chunks = pair_ssem.shape[1]
    step = tables // chunks
    me = lax.axis_index("rows")
    col = lax.axis_index("cols")
    hi, lo = me // 2, me % 2
    mate = hi * 2 + (1 - lo)

    sources = (counts_hbm, rows_hbm, examples_hbm, tables_hbm, dense_hbm)
    targets = (counts_ref, rows_ref, examples_ref, table_buf, dense_ref)
    loads = [pltpu.make_async_copy(a, b, load_sem.at[i]) for i, (a, b) in enumerate(zip(sources, targets))]

    barrier = pltpu.get_barrier_semaphore()
    for j in range(1, n):
        pl.semaphore_signal(barrier, inc=1, device_id={"rows": (me + j) % n}, device_id_type=MESH)
    for j in range(1, cols):
        pl.semaphore_signal(barrier, inc=1, device_id={"cols": (col + j) % cols}, device_id_type=MESH)

    for load in loads:
        load.start()

    slot = lax.broadcasted_iota(jnp.int32, (tables, cap), 1)
    table_id = lax.broadcasted_iota(jnp.int32, (tables, cap), 0)
    for load in loads[:3]:
        load.wait()
    for p in range(n):
        count = jnp.full((tables, cap), counts_ref[0, 0, p], jnp.int32)
        for t in range(1, tables):
            count = jnp.where(table_id == t, counts_ref[0, t, p], count)
        rows_p = rows_ref[0, p]
        ex_p = jnp.where(slot < count, examples_ref[0, p], DEAD)
        id_send[p, 0:tables, :] = jnp.concatenate([rows_p, rows_p], axis=1)
        id_send[p, tables : 2 * tables, :] = jnp.concatenate([ex_p, ex_p], axis=1)

    pl.semaphore_wait(barrier, n - 1 + cols - 1)

    high_half = (2 * hi) // far
    low_hi = hi * (1 - high_half) + (far - 1 - hi) * high_half

    def group_of(k):
        beyond = (2 * (far - 1) - k - low_hi) // far
        g = far - 2 - k + beyond
        return g * (1 - high_half) + (far - 1 - g) * high_half

    def id_copy(dst):
        return pltpu.make_async_remote_copy(
            src_ref=id_send.at[dst],
            dst_ref=id_recv.at[me],
            send_sem=id_ssem.at[dst],
            recv_sem=id_rsem.at[me],
            device_id={"rows": dst},
            device_id_type=MESH,
        )

    def id_wait(src):
        pltpu.make_async_remote_copy(
            src_ref=id_send.at[src],
            dst_ref=id_recv.at[src],
            send_sem=id_ssem.at[src],
            recv_sem=id_rsem.at[src],
            device_id={"rows": src},
            device_id_type=MESH,
        ).wait_recv()

    for k in range(far - 1):
        dst_hi = group_of(k)
        id_copy(dst_hi * 2 + lo).start()
        id_copy(dst_hi * 2 + (1 - lo)).start()
    id_copy(mate).start()
    id_recv[me] = id_send[me]

    loads[3].wait()
    for t in range(tables):
        whole = table_buf[t]
        high = whole.astype(jnp.bfloat16)
        split_buf[t, :, 0:width] = high
        split_buf[t, :, width : 2 * width] = (whole - high.astype(jnp.float32)).astype(jnp.bfloat16)

    first_half = lax.broadcasted_iota(jnp.int32, (tables, 2 * cap), 1) < cap
    offset = jnp.where(first_half, lo * here, (1 - lo) * here)
    row_iota = lax.broadcasted_iota(jnp.int32, (range_rows, 2 * cap), 0)
    ex_iota = lax.broadcasted_iota(jnp.int32, (2 * here, 2 * cap), 0)

    def pair_copy(g, c):
        piece = pl.ds(c * step, step)
        return pltpu.make_async_remote_copy(
            src_ref=pair_send.at[g, piece],
            dst_ref=pair_recv.at[g, piece],
            send_sem=pair_ssem.at[g, c],
            recv_sem=pair_rsem.at[g, c],
            device_id={"rows": mate},
            device_id_type=MESH,
        )

    def far_copy(g, c):
        piece = pl.ds(c * step, step)
        return pltpu.make_async_remote_copy(
            src_ref=far_send.at[g, piece],
            dst_ref=far_recv.at[hi, piece],
            send_sem=far_ssem.at[g, c],
            recv_sem=far_rsem.at[hi, c],
            device_id={"rows": g * 2 + lo},
            device_id_type=MESH,
        )

    def far_wait(g, c):
        piece = pl.ds(c * step, step)
        pltpu.make_async_remote_copy(
            src_ref=far_send.at[g, piece],
            dst_ref=far_recv.at[g, piece],
            send_sem=far_ssem.at[g, c],
            recv_sem=far_rsem.at[g, c],
            device_id={"rows": g * 2 + lo},
            device_id_type=MESH,
        ).wait_recv()

    def compute(g):
        even = id_recv[g * 2]
        odd = id_recv[g * 2 + 1]
        row_of = jnp.where(first_half, even[0:tables], odd[0:tables])
        code = jnp.where(first_half, even[tables : 2 * tables], odd[tables : 2 * tables]) + offset
        for t in range(tables):
            row_hot = jnp.where(row_iota == row_of[t : t + 1], 1.0, 0.0).astype(jnp.bfloat16)
            ex_hot = jnp.where(ex_iota == code[t : t + 1], 1.0, 0.0).astype(jnp.bfloat16)
            hits = lax.dot_general(
                ex_hot, row_hot, (((1,), (1,)), ((), ())), preferred_element_type=jnp.float32
            ).astype(jnp.bfloat16)
            both = jnp.dot(hits, split_buf[t], preferred_element_type=jnp.float32)
            part = both[:, 0:width] + both[:, width : 2 * width]
            pair_keep[g, t] = part[0:here]
            pair_send[g, t] = part[here : 2 * here]
            if (t + 1) % step == 0:
                pair_copy(g, t // step).start()

    def forward(g):
        for c in range(chunks):
            pair_copy(g, c).wait_recv()
            piece = pl.ds(c * step, step)
            far_send[g, piece] = pair_keep[g, piece] + pair_recv[g, piece]
            far_copy(g, c).start()

    def remote_group(g):
        id_wait(g * 2)
        id_wait(g * 2 + 1)
        compute(g)

    remote_group(group_of(0))
    if far <= 8:
        for k in range(1, far - 1):
            remote_group(group_of(k))
            forward(group_of(k - 1))
    else:

        @pl.loop(1, far - 1)
        def _(k):
            remote_group(group_of(k))
            forward(group_of(k - 1))

    id_wait(mate)
    compute(hi)
    forward(group_of(far - 2))

    for c in range(chunks):
        pair_copy(hi, c).wait_recv()
    total = pair_keep[hi] + pair_recv[hi]
    for k in range(far - 1):
        g = group_of(far - 2 - k)
        for c in range(chunks):
            far_wait(g, c)
        total = total + far_recv[g]

    for t in range(tables):
        pooled_ref[:, t, :] = total[t]
    loads[4].wait()
    vectors = [dense_ref[...]] + [total[t] for t in range(tables)]
    lane = lax.broadcasted_iota(jnp.int32, (here, 128), 1)
    gram = jnp.zeros((here, 128), jnp.float32)
    pair = 0
    for i in range(tables + 1):
        for j in range(i + 1, tables + 1):
            inner = jnp.sum(vectors[i] * vectors[j], axis=1, keepdims=True)
            gram = jnp.where(lane == pair, inner, gram)
            pair += 1
    gram = gram.T[0 : gram_send.shape[0]]
    gram_send[...] = gram
    gram_recv[col] = gram

    def gram_copy(j):
        return pltpu.make_async_remote_copy(
            src_ref=gram_send,
            dst_ref=gram_recv.at[col],
            send_sem=gram_ssem.at[j],
            recv_sem=gram_rsem.at[col],
            device_id={"cols": (col + j) % cols},
            device_id_type=MESH,
        )

    for j in range(1, cols):
        gram_copy(j).start()
    for j in range(1, cols):
        src = (col + j) % cols
        pltpu.make_async_remote_copy(
            src_ref=gram_send,
            dst_ref=gram_recv.at[src],
            send_sem=gram_ssem.at[j],
            recv_sem=gram_rsem.at[src],
            device_id={"cols": src},
            device_id_type=MESH,
        ).wait_recv()
    summed = gram_recv[0]
    for c in range(1, cols):
        summed = summed + gram_recv[c]
    inter_ref[...] = (summed * (width * cols) ** (-0.5))[0:pair]

    for j in range(1, n):
        id_copy((me + j) % n).wait_send()
    for c in range(chunks):
        for g in range(far):
            pair_copy(g, c).wait_send()
        for j in range(1, far):
            far_copy((hi + j) % far, c).wait_send()
    for j in range(1, cols):
        gram_copy(j).wait_send()


def body(n, cols, tables, dense_features, slot_rows, slot_examples, slot_counts):
    count, range_rows, width = tables.shape
    here = dense_features.shape[0]
    cap = slot_rows.shape[3]
    far = n // 2
    pairs = (count + 1) * count // 2
    vmem = pl.BlockSpec(memory_space=pltpu.VMEM)
    block = (far, count, here, width)
    chunks = CHUNKS
    any_space = pl.BlockSpec(memory_space=pl.ANY)
    pair_rows = -(-pairs // 8) * 8
    pooled, inter = pl.pallas_call(
        functools.partial(kernel, n, cols),
        out_shape=(
            pltpu.VMEM((here, count, width), jnp.float32),
            pltpu.VMEM((pairs, here), jnp.float32),
        ),
        in_specs=[any_space] * 5,
        out_specs=(vmem, vmem),
        scratch_shapes=[
            pltpu.VMEM((here, width), jnp.float32),
            pltpu.VMEM(slot_rows.shape, jnp.int32),
            pltpu.VMEM(slot_rows.shape, jnp.int32),
            pltpu.SMEM((1, count, n), jnp.int32),
            pltpu.VMEM((count, range_rows, width), jnp.float32),
            pltpu.VMEM((count, range_rows, 2 * width), jnp.bfloat16),
            pltpu.VMEM((n, 2 * count, 2 * cap), jnp.int32),
            pltpu.VMEM((n, 2 * count, 2 * cap), jnp.int32),
            pltpu.VMEM(block, jnp.float32),
            pltpu.VMEM(block, jnp.float32),
            pltpu.VMEM(block, jnp.float32),
            pltpu.VMEM(block, jnp.float32),
            pltpu.VMEM(block, jnp.float32),
            pltpu.VMEM((cols, pair_rows, here), jnp.float32),
            pltpu.VMEM((pair_rows, here), jnp.float32),
            pltpu.SemaphoreType.DMA((5,)),
            pltpu.SemaphoreType.DMA((n,)),
            pltpu.SemaphoreType.DMA((n,)),
            pltpu.SemaphoreType.DMA((far, chunks)),
            pltpu.SemaphoreType.DMA((far, chunks)),
            pltpu.SemaphoreType.DMA((far, chunks)),
            pltpu.SemaphoreType.DMA((far, chunks)),
            pltpu.SemaphoreType.DMA((cols,)),
            pltpu.SemaphoreType.DMA((cols,)),
        ],
        compiler_params=pltpu.CompilerParams(collective_id=0, has_side_effects=True),
    )(tables, dense_features, slot_rows, slot_examples, slot_counts.transpose(0, 2, 1))
    return pooled, inter.T


def solution(mesh):
    placed = (
        P(None, "rows", "cols"),
        P("rows", "cols"),
        P("rows", None, None, None),
        P("rows", None, None, None),
        P("rows", None, None),
    )
    return jax.shard_map(
        functools.partial(body, mesh.shape["rows"], mesh.shape["cols"]),
        mesh=mesh,
        in_specs=placed,
        out_specs=(P("rows", None, "cols"), P("rows", None)),
        check_vma=False,
    )
```

```python
import functools

import jax
import jax.numpy as jnp
from jax import lax
from jax.experimental import pallas as pl
from jax.experimental.pallas import tpu as pltpu
from jax.sharding import PartitionSpec as P

MESH = pl.DeviceIdType.MESH
CHUNKS = 2
DEAD = -65536


def kernel(
    n,
    cols,
    tables_hbm,
    dense_hbm,
    rows_hbm,
    examples_hbm,
    counts_hbm,
    pooled_ref,
    inter_ref,
    dense_ref,
    rows_ref,
    examples_ref,
    counts_ref,
    table_buf,
    split_buf,
    id_send,
    id_recv,
    pair_keep,
    pair_send,
    pair_recv,
    far_send,
    far_recv,
    near_recv,
    gram_recv,
    gram_send,
    load_sem,
    id_ssem,
    id_rsem,
    pair_ssem,
    pair_rsem,
    far_ssem,
    far_rsem,
    near_ssem,
    near_rsem,
    gram_ssem,
    gram_rsem,
):
    tables, range_rows, width = table_buf.shape
    here = dense_ref.shape[0]
    cap = rows_ref.shape[3]
    far = n // 2
    chunks = pair_ssem.shape[1]
    step = tables // chunks
    me = lax.axis_index("rows")
    col = lax.axis_index("cols")
    hi, lo = me // 2, me % 2
    mate = hi * 2 + (1 - lo)

    sources = (counts_hbm, rows_hbm, examples_hbm, tables_hbm, dense_hbm)
    targets = (counts_ref, rows_ref, examples_ref, table_buf, dense_ref)
    loads = [pltpu.make_async_copy(a, b, load_sem.at[i]) for i, (a, b) in enumerate(zip(sources, targets))]

    barrier = pltpu.get_barrier_semaphore()
    for j in range(1, n):
        pl.semaphore_signal(barrier, inc=1, device_id={"rows": (me + j) % n}, device_id_type=MESH)
    for j in range(1, cols):
        pl.semaphore_signal(barrier, inc=1, device_id={"cols": (col + j) % cols}, device_id_type=MESH)

    for load in loads:
        load.start()

    slot = lax.broadcasted_iota(jnp.int32, (tables, cap), 1)
    table_id = lax.broadcasted_iota(jnp.int32, (tables, cap), 0)
    for load in loads[:3]:
        load.wait()
    for p in range(n):
        count = jnp.full((tables, cap), counts_ref[0, 0, p], jnp.int32)
        for t in range(1, tables):
            count = jnp.where(table_id == t, counts_ref[0, t, p], count)
        rows_p = rows_ref[0, p]
        ex_p = jnp.where(slot < count, examples_ref[0, p], DEAD)
        id_send[p, 0:tables, :] = jnp.concatenate([rows_p, rows_p], axis=1)
        id_send[p, tables : 2 * tables, :] = jnp.concatenate([ex_p, ex_p], axis=1)

    pl.semaphore_wait(barrier, n - 1 + cols - 1)

    def group_of(k):
        return (hi // 2 + 1 + k // 2) % (far // 2) * 2 + (hi + 1 + k) % 2

    def id_copy(dst):
        return pltpu.make_async_remote_copy(
            src_ref=id_send.at[dst],
            dst_ref=id_recv.at[me],
            send_sem=id_ssem.at[dst],
            recv_sem=id_rsem.at[me],
            device_id={"rows": dst},
            device_id_type=MESH,
        )

    def id_wait(src):
        pltpu.make_async_remote_copy(
            src_ref=id_send.at[src],
            dst_ref=id_recv.at[src],
            send_sem=id_ssem.at[src],
            recv_sem=id_rsem.at[src],
            device_id={"rows": src},
            device_id_type=MESH,
        ).wait_recv()

    for k in range(far - 1):
        dst_hi = group_of(k)
        id_copy(dst_hi * 2 + lo).start()
        id_copy(dst_hi * 2 + (1 - lo)).start()
    id_copy(mate).start()
    id_recv[me] = id_send[me]

    loads[3].wait()
    for t in range(tables):
        whole = table_buf[t]
        high = whole.astype(jnp.bfloat16)
        split_buf[t, :, 0:width] = high
        split_buf[t, :, width : 2 * width] = (whole - high.astype(jnp.float32)).astype(jnp.bfloat16)

    first_half = lax.broadcasted_iota(jnp.int32, (tables, 2 * cap), 1) < cap
    offset = jnp.where(first_half, lo * here, (1 - lo) * here)
    row_iota = lax.broadcasted_iota(jnp.int32, (range_rows, 2 * cap), 0)
    ex_iota = lax.broadcasted_iota(jnp.int32, (2 * here, 2 * cap), 0)

    def pair_copy(g, c):
        piece = pl.ds(c * step, step)
        return pltpu.make_async_remote_copy(
            src_ref=pair_send.at[g, piece],
            dst_ref=pair_recv.at[g, piece],
            send_sem=pair_ssem.at[g, c],
            recv_sem=pair_rsem.at[g, c],
            device_id={"rows": mate},
            device_id_type=MESH,
        )

    def far_copy(g, c):
        piece = pl.ds(c * step, step)
        return pltpu.make_async_remote_copy(
            src_ref=far_send.at[g, piece],
            dst_ref=far_recv.at[hi, piece],
            send_sem=far_ssem.at[g, c],
            recv_sem=far_rsem.at[hi, c],
            device_id={"rows": g * 2 + lo},
            device_id_type=MESH,
        )

    def far_wait(g, c):
        piece = pl.ds(c * step, step)
        pltpu.make_async_remote_copy(
            src_ref=far_send.at[g, piece],
            dst_ref=far_recv.at[g, piece],
            send_sem=far_ssem.at[g, c],
            recv_sem=far_rsem.at[g, c],
            device_id={"rows": g * 2 + lo},
            device_id_type=MESH,
        ).wait_recv()

    near = hi + 1 - 2 * (hi % 2)

    def near_copy(same):
        return pltpu.make_async_remote_copy(
            src_ref=pair_keep.at[near] if same else pair_send.at[near],
            dst_ref=near_recv.at[0 if same else 1],
            send_sem=near_ssem.at[0 if same else 1],
            recv_sem=near_rsem.at[0 if same else 1],
            device_id={"rows": near * 2 + (lo if same else 1 - lo)},
            device_id_type=MESH,
        )

    def compute(g, paired=True):
        even = id_recv[g * 2]
        odd = id_recv[g * 2 + 1]
        row_of = jnp.where(first_half, even[0:tables], odd[0:tables])
        code = jnp.where(first_half, even[tables : 2 * tables], odd[tables : 2 * tables]) + offset
        for t in range(tables):
            row_hot = jnp.where(row_iota == row_of[t : t + 1], 1.0, 0.0).astype(jnp.bfloat16)
            ex_hot = jnp.where(ex_iota == code[t : t + 1], 1.0, 0.0).astype(jnp.bfloat16)
            hits = lax.dot_general(
                ex_hot, row_hot, (((1,), (1,)), ((), ())), preferred_element_type=jnp.float32
            ).astype(jnp.bfloat16)
            both = jnp.dot(hits, split_buf[t], preferred_element_type=jnp.float32)
            part = both[:, 0:width] + both[:, width : 2 * width]
            pair_keep[g, t] = part[0:here]
            pair_send[g, t] = part[here : 2 * here]
            if paired and (t + 1) % step == 0:
                pair_copy(g, t // step).start()

    def forward(g):
        for c in range(chunks):
            pair_copy(g, c).wait_recv()
            piece = pl.ds(c * step, step)
            far_send[g, piece] = pair_keep[g, piece] + pair_recv[g, piece]
            far_copy(g, c).start()

    def remote_group(g):
        id_wait(g * 2)
        id_wait(g * 2 + 1)
        compute(g)

    remote_group(group_of(0))
    if far <= 8:
        for k in range(1, far - 2):
            remote_group(group_of(k))
            forward(group_of(k - 1))
    else:

        @pl.loop(1, far - 2)
        def _(k):
            remote_group(group_of(k))
            forward(group_of(k - 1))

    id_wait(near * 2)
    id_wait(near * 2 + 1)
    compute(near, False)
    near_copy(True).start()
    near_copy(False).start()
    forward(group_of(far - 3))
    id_wait(mate)
    compute(hi)

    for c in range(chunks):
        pair_copy(hi, c).wait_recv()
    total = pair_keep[hi] + pair_recv[hi]
    for same in (True, False):
        near_copy(same).wait_recv()
    total = total + (near_recv[0] + near_recv[1])
    for k in range(far - 2):
        g = group_of(far - 3 - k)
        for c in range(chunks):
            far_wait(g, c)
        total = total + far_recv[g]

    for t in range(tables):
        pooled_ref[:, t, :] = total[t]
    loads[4].wait()
    vectors = [dense_ref[...]] + [total[t] for t in range(tables)]
    lane = lax.broadcasted_iota(jnp.int32, (here, 128), 1)
    gram = jnp.zeros((here, 128), jnp.float32)
    pair = 0
    for i in range(tables + 1):
        for j in range(i + 1, tables + 1):
            inner = jnp.sum(vectors[i] * vectors[j], axis=1, keepdims=True)
            gram = jnp.where(lane == pair, inner, gram)
            pair += 1
    gram = gram.T[0 : gram_send.shape[0]]
    gram_send[...] = gram
    gram_recv[col] = gram

    def gram_copy(j):
        return pltpu.make_async_remote_copy(
            src_ref=gram_send,
            dst_ref=gram_recv.at[col],
            send_sem=gram_ssem.at[j],
            recv_sem=gram_rsem.at[col],
            device_id={"cols": (col + j) % cols},
            device_id_type=MESH,
        )

    for j in range(1, cols):
        gram_copy(j).start()
    for j in range(1, cols):
        src = (col + j) % cols
        pltpu.make_async_remote_copy(
            src_ref=gram_send,
            dst_ref=gram_recv.at[src],
            send_sem=gram_ssem.at[j],
            recv_sem=gram_rsem.at[src],
            device_id={"cols": src},
            device_id_type=MESH,
        ).wait_recv()
    summed = gram_recv[0]
    for c in range(1, cols):
        summed = summed + gram_recv[c]
    inter_ref[...] = (summed * (width * cols) ** (-0.5))[0:pair]

    for j in range(1, n):
        id_copy((me + j) % n).wait_send()
    for c in range(chunks):
        pair_copy(hi, c).wait_send()
        for k in range(far - 2):
            pair_copy(group_of(k), c).wait_send()
            far_copy(group_of(k), c).wait_send()
    for same in (True, False):
        near_copy(same).wait_send()
    for j in range(1, cols):
        gram_copy(j).wait_send()


def body(n, cols, tables, dense_features, slot_rows, slot_examples, slot_counts):
    count, range_rows, width = tables.shape
    here = dense_features.shape[0]
    cap = slot_rows.shape[3]
    far = n // 2
    pairs = (count + 1) * count // 2
    vmem = pl.BlockSpec(memory_space=pltpu.VMEM)
    block = (far, count, here, width)
    chunks = CHUNKS
    any_space = pl.BlockSpec(memory_space=pl.ANY)
    pair_rows = -(-pairs // 8) * 8
    pooled, inter = pl.pallas_call(
        functools.partial(kernel, n, cols),
        out_shape=(
            pltpu.VMEM((here, count, width), jnp.float32),
            pltpu.VMEM((pairs, here), jnp.float32),
        ),
        in_specs=[any_space] * 5,
        out_specs=(vmem, vmem),
        scratch_shapes=[
            pltpu.VMEM((here, width), jnp.float32),
            pltpu.VMEM(slot_rows.shape, jnp.int32),
            pltpu.VMEM(slot_rows.shape, jnp.int32),
            pltpu.SMEM((1, count, n), jnp.int32),
            pltpu.VMEM((count, range_rows, width), jnp.float32),
            pltpu.VMEM((count, range_rows, 2 * width), jnp.bfloat16),
            pltpu.VMEM((n, 2 * count, 2 * cap), jnp.int32),
            pltpu.VMEM((n, 2 * count, 2 * cap), jnp.int32),
            pltpu.VMEM(block, jnp.float32),
            pltpu.VMEM(block, jnp.float32),
            pltpu.VMEM(block, jnp.float32),
            pltpu.VMEM(block, jnp.float32),
            pltpu.VMEM(block, jnp.float32),
            pltpu.VMEM((2,) + block[1:], jnp.float32),
            pltpu.VMEM((cols, pair_rows, here), jnp.float32),
            pltpu.VMEM((pair_rows, here), jnp.float32),
            pltpu.SemaphoreType.DMA((5,)),
            pltpu.SemaphoreType.DMA((n,)),
            pltpu.SemaphoreType.DMA((n,)),
            pltpu.SemaphoreType.DMA((far, chunks)),
            pltpu.SemaphoreType.DMA((far, chunks)),
            pltpu.SemaphoreType.DMA((far, chunks)),
            pltpu.SemaphoreType.DMA((far, chunks)),
            pltpu.SemaphoreType.DMA((2,)),
            pltpu.SemaphoreType.DMA((2,)),
            pltpu.SemaphoreType.DMA((cols,)),
            pltpu.SemaphoreType.DMA((cols,)),
        ],
        compiler_params=pltpu.CompilerParams(collective_id=0, has_side_effects=True),
    )(tables, dense_features, slot_rows, slot_examples, slot_counts.transpose(0, 2, 1))
    return pooled, inter.T


def solution(mesh):
    placed = (
        P(None, "rows", "cols"),
        P("rows", "cols"),
        P("rows", None, None, None),
        P("rows", None, None, None),
        P("rows", None, None),
    )
    return jax.shard_map(
        functools.partial(body, mesh.shape["rows"], mesh.shape["cols"]),
        mesh=mesh,
        in_specs=placed,
        out_specs=(P("rows", None, "cols"), P("rows", None)),
        check_vma=False,
    )
```
